32 devices in a mesh: samp: 16 (over z, y, core), snp: 2 (over x).
Axes of the slice: x: 2, y: 2, z: 4, core: 2. Of those that a mesh axis runs over, the one named last changes fastest.
Arguments:
- genotype: int32 [16384, 4096], P('samp', 'snp'), may hold values from 0 to 3, as said below
- basis: bfloat16 [4096, 40], P('snp'), may hold values from -6 to 6
Outputs:
- sample_scores: bfloat16 [16384, 40], P('samp')
- snp_block: float32 [4096, 40], P('snp')
The draws below stay inside these ranges and needn't reach their ends.
Inputs may be any that keep to these rules, and one draw needn't show every extreme that they name: `genotype`: the value 3 marks a missing call; 0, 1 and 2 are dosages.
All inputs are finite; a program needn't handle non-finite values.
Results may differ from the reference program's by a relative error of at most 0.0065.
Values may be sent and summed in bfloat16 or wider, within the bound.
A program may use at most 64 MiB of HBM per device.

```python
import jax
import jax.numpy as jnp
from jax import lax

M = 4096
K = 40
ITERS = 2
NS = 16384


def draw_genotype(key, part):
    key_base = jax.random.fold_in(key, 11)
    key_factor = jax.random.fold_in(key, 15)
    key_member = jax.random.fold_in(key, 16)
    key_first = jax.random.fold_in(key, 12)
    key_second = jax.random.fold_in(key, 13)
    key_missing = jax.random.fold_in(key, 14)
    base = jax.random.randint(key_base, (M,), 50, 300)
    cluster_factor = jax.random.randint(key_factor, (48, M), 250, 1750)
    table = base[None, :] * cluster_factor // 1000
    member = jax.random.randint(key_member, (NS,), 0, 48)
    thresh = table[member]
    first = jax.random.randint(key_first, (NS, M), 0, 1000)
    second = jax.random.randint(key_second, (NS, M), 0, 1000)
    dosage = (first < thresh).astype(jnp.int32) + (second < thresh).astype(jnp.int32)
    position = jnp.arange(NS, dtype=jnp.int32)
    keep_level = 300 + 600 * position // NS
    missing = jax.random.randint(key_missing, (NS, M), 0, 1000) >= keep_level[:, None]
    return jnp.where(missing, 3, dosage).astype(jnp.int32)


def level_of(key, dims, split, least, high):
    loudness, own = 1.0, jax.random.fold_in(key, 6)
    for axis_at, shards_of in split:
        steps = jnp.exp(jax.random.uniform(jax.random.fold_in(own, axis_at), (shards_of,), jnp.float32, least / len(split), high / len(split)))
        loudness = loudness * jnp.repeat(steps, dims[axis_at] // shards_of).reshape([-1 if axis == axis_at else 1 for axis in range(len(dims))])
    return loudness


def scatter_about(own_key, dims, scale, reach, cuts=(), kind=jnp.bfloat16):
    loudness = level_of(own_key, dims, cuts, -0.22, 0.18) if cuts else 1.0
    values = jax.random.normal(own_key, dims, jnp.float32) * scale * loudness
    return jnp.minimum(jnp.maximum(values, -reach), reach).astype(kind)


def setup_inputs(seed: int = 0) -> dict:
    key_of = jax.random.split(jax.random.key(seed), 3)
    return {
        "genotype": draw_genotype(jax.random.fold_in(key_of[2], 71), 0),
        "basis": scatter_about(key_of[1], (M, K), 1.0, 6.0, ((0, 2),)),
    }


def reference(genotype, basis):
    observed = genotype < 3
    dosage = jnp.where(observed, genotype, 0).astype(jnp.float32)
    allele_sum = lax.optimization_barrier(jnp.sum(dosage, axis=0))
    called = lax.optimization_barrier(jnp.sum(observed.astype(jnp.float32), axis=0))
    freq = (allele_sum + 1.0) / (2.0 * called + 2.0)
    scale = 1.0 / jnp.sqrt(2.0 * freq * (1.0 - freq))
    standard = jnp.where(observed, (dosage - 2.0 * freq) * scale, 0.0).astype(jnp.bfloat16)
    block = basis
    for step in range(ITERS):
        scores = jnp.dot(standard, block, preferred_element_type=jnp.float32)
        sample_scores = scores.astype(jnp.bfloat16)
        snp_block = jnp.dot(standard.T, sample_scores, preferred_element_type=jnp.float32) / NS
        block = snp_block.astype(jnp.bfloat16)
    return (sample_scores, snp_block)
```

```python
import functools

import jax
import jax.numpy as jnp
from jax import lax
from jax.experimental import pallas as pl
from jax.experimental.pallas import tpu as pltpu
from jax.sharding import PartitionSpec as P

ITERS = 2
LANES = 128
WIDE = 256
SHIFT = 65536
MESH = pl.DeviceIdType.MESH
NT = (((1,), (1,)), ((), ()))


def flipped(me, bits):
    out, step = me, 1
    while step <= bits:
        if bits & step:
            out = out + step * (1 - 2 * lax.rem(me // step, 2))
        step *= 2
    return out


def kernel(
    n, genotype, basis, scores_out, block_out,
    raw, std, stat, table, start, acc, mine, theirs, part, got, full, result,
    load_sem, in_sem, stat_send, stat_recv, score_send, score_recv,
    part_send, part_recv, full_send, full_recv, out_sem,
):
    me = lax.axis_index("samp")
    side = lax.axis_index("snp")
    rows, cols = genotype.shape
    total = rows * n
    blocks = cols // LANES
    groups = blocks // 8
    chunks = cols // WIDE

    barrier = pltpu.get_barrier_semaphore()
    for d in range(1, n):
        pl.semaphore_signal(barrier, inc=1, device_id={"samp": flipped(me, d)}, device_id_type=MESH)
    pl.semaphore_signal(barrier, inc=1, device_id={"snp": 1 - side}, device_id_type=MESH)

    def load(c):
        at = pl.ds(pl.multiple_of(c * WIDE, WIDE), WIDE)
        return pltpu.make_async_copy(genotype.at[:, at], raw.at[:, at], load_sem.at[c])

    for c in range(chunks):
        load(c).start()
    fetch = pltpu.make_async_copy(basis, start, in_sem)
    fetch.start()

    def count(c, _):
        load(c).wait()
        for half in range(WIDE // LANES):
            at = pl.ds(pl.multiple_of(c * WIDE + half * LANES, LANES), LANES)
            g = raw[:, at]
            sums = jnp.sum(jnp.where(g == 3, SHIFT, g), axis=0, keepdims=True)
            std[:, at] = g.astype(jnp.float32).astype(jnp.bfloat16)
            j = c * (WIDE // LANES) + half
            stat[me, j // 8, pl.ds(lax.rem(j, 8), 1), :] = sums
        return 0

    def stat_copy(h, d):
        peer = flipped(me, d)
        return pltpu.make_async_remote_copy(
            src_ref=stat.at[me, h], dst_ref=stat.at[me, h],
            send_sem=stat_send.at[h, d], recv_sem=stat_recv.at[h, d],
            device_id={"samp": peer}, device_id_type=MESH,
        )

    per_group = chunks // groups
    for h in range(groups):
        lax.fori_loop(h * per_group, (h + 1) * per_group, count, 0)
        if h == 0:
            pl.semaphore_wait(barrier, n)
        for d in reversed(range(1, n)):
            stat_copy(h, d).start()

    for h in range(groups):
        for d in range(1, n):
            stat_copy(h, d).wait_recv()
        packed = stat[0, h]
        for s in range(1, n):
            packed += stat[s, h]
        missing = packed // SHIFT
        allele_sum = (packed - missing * SHIFT).astype(jnp.float32)
        called = (total - missing).astype(jnp.float32)
        freq = (allele_sum + 1.0) / (2.0 * called + 2.0)
        scale = 1.0 / jnp.sqrt(2.0 * freq * (1.0 - freq))
        for k in range(3):
            table[k, h] = (float(k) - 2.0 * freq) * scale

    fetch.wait()
    zero = jnp.zeros((), jnp.bfloat16)

    def standardize(j):
        at = pl.ds(pl.multiple_of(j * LANES, LANES), LANES)
        g = std[:, at]
        row = [
            jnp.broadcast_to(
                table[k, j // 8, pl.ds(lax.rem(j, 8), 1), :].astype(jnp.bfloat16), g.shape
            )
            for k in range(3)
        ]
        std[:, at] = jnp.where(
            g == 0, row[0], jnp.where(g == 1, row[1], jnp.where(g == 2, row[2], zero))
        )

    acc[...] = jnp.zeros_like(acc)

    def first(c, _):
        for half in range(WIDE // LANES):
            standardize(c * (WIDE // LANES) + half)
        at = pl.ds(pl.multiple_of(c * WIDE, WIDE), WIDE)
        acc[...] += lax.dot_general(start[:, at], std[:, at], NT, preferred_element_type=jnp.float32)
        return 0

    lax.fori_loop(0, chunks, first, 0)

    for step in range(ITERS):
        last = step == ITERS - 1
        mine[step] = acc[...].astype(jnp.bfloat16)
        swap = pltpu.make_async_remote_copy(
            src_ref=mine.at[step], dst_ref=theirs.at[step],
            send_sem=score_send.at[step], recv_sem=score_recv.at[step],
            device_id={"snp": 1 - side}, device_id_type=MESH,
        )
        swap.start()
        swap.wait_recv()
        scores = (mine[step].astype(jnp.float32) + theirs[step].astype(jnp.float32)).astype(jnp.bfloat16)
        result[...] = scores
        if last:
            score_write = pltpu.make_async_copy(result, scores_out, out_sem.at[0])
            score_write.start()

        def part_copy(owner):
            return pltpu.make_async_remote_copy(
                src_ref=part.at[step, owner], dst_ref=got.at[step, me],
                send_sem=part_send.at[step, owner], recv_sem=part_recv.at[step, me],
                device_id={"samp": owner}, device_id_type=MESH,
            )

        def part_arrival(sender):
            return pltpu.make_async_remote_copy(
                src_ref=part.at[step, sender], dst_ref=got.at[step, sender],
                send_sem=part_send.at[step, sender], recv_sem=part_recv.at[step, sender],
                device_id={"samp": sender}, device_id_type=MESH,
            )

        per_dot = 4 if n % 4 == 0 else 1
        dots = n // per_dot

        def back(i, _):
            c = lax.rem(me // per_dot + 1 + i, dots)
            at = pl.ds(pl.multiple_of(c * (per_dot * LANES), per_dot * LANES), per_dot * LANES)
            local = jnp.dot(result[...], std[:, at], preferred_element_type=jnp.float32)
            for r in range(per_dot):
                owner = c * per_dot + r
                part[step, owner] = local[:, r * LANES : (r + 1) * LANES].astype(jnp.bfloat16)

                @pl.when(owner != me)
                def _():
                    part_copy(owner).start()

            return 0

        lax.fori_loop(0, dots, back, 0)

        whole = part[step, me].astype(jnp.float32)
        for d in range(1, n):
            sender = flipped(me, d)
            part_arrival(sender).wait_recv()
            whole += got[step, sender].astype(jnp.float32)
        full[step, me] = (whole / total).astype(jnp.bfloat16)

        def full_copy(peer, slot):
            return pltpu.make_async_remote_copy(
                src_ref=full.at[step, slot], dst_ref=full.at[step, slot],
                send_sem=full_send.at[step, peer], recv_sem=full_recv.at[step, slot],
                device_id={"samp": peer}, device_id_type=MESH,
            )

        for d in reversed(range(1, n)):
            full_copy(flipped(me, d), me).start()

        if not last:
            acc[...] = jnp.zeros_like(acc)

        def arrive(s):
            @pl.when(s != me)
            def _():
                full_copy(s, s).wait_recv()

        def take(i, _):
            c = lax.rem(me // 2 + i, n // 2)
            for r in range(2):
                arrive(2 * c + r)
            at = pl.ds(pl.multiple_of(c * WIDE, WIDE), WIDE)
            both = jnp.concatenate([full[step, 2 * c], full[step, 2 * c + 1]], axis=1)
            if last:
                block_out[:, at] = both.astype(jnp.float32)
            else:
                acc[...] += lax.dot_general(both, std[:, at], NT, preferred_element_type=jnp.float32)
            return 0

        lax.fori_loop(0, n // 2, take, 0)

        for d in range(1, n):
            peer = flipped(me, d)
            part_copy(peer).wait_send()
            full_copy(peer, me).wait_send()
        swap.wait_send()

    for h in range(groups):
        for d in range(1, n):
            stat_copy(h, d).wait_send()
    score_write.wait()


def fused(n, genotype, basis):
    rows, cols = genotype.shape
    width = basis.shape[1]
    blocks = cols // LANES
    dma = pltpu.SemaphoreType.DMA
    scores, block = pl.pallas_call(
        functools.partial(kernel, n),
        out_shape=(
            jax.ShapeDtypeStruct((width, rows), jnp.bfloat16),
            jax.ShapeDtypeStruct((width, cols), jnp.float32),
        ),
        in_specs=[pl.BlockSpec(memory_space=pl.ANY)] * 2,
        out_specs=(
            pl.BlockSpec(memory_space=pl.ANY),
            pl.BlockSpec(memory_space=pltpu.VMEM),
        ),
        scratch_shapes=[
            pltpu.VMEM((rows, cols), jnp.int32),
            pltpu.VMEM((rows, cols), jnp.bfloat16),
            pltpu.VMEM((n, blocks // 8, 8, LANES), jnp.int32),
            pltpu.VMEM((3, blocks // 8, 8, LANES), jnp.float32),
            pltpu.VMEM((width, cols), jnp.bfloat16),
            pltpu.VMEM((width, rows), jnp.float32),
            pltpu.VMEM((ITERS, width, rows), jnp.bfloat16),
            pltpu.VMEM((ITERS, width, rows), jnp.bfloat16),
            pltpu.VMEM((ITERS, n, width, LANES), jnp.bfloat16),
            pltpu.VMEM((ITERS, n, width, LANES), jnp.bfloat16),
            pltpu.VMEM((ITERS, n, width, LANES), jnp.bfloat16),
            pltpu.VMEM((width, rows), jnp.bfloat16),
            dma((cols // WIDE,)),
            dma,
            dma((blocks // 8, n)),
            dma((blocks // 8, n)),
            dma((ITERS,)),
            dma((ITERS,)),
            dma((ITERS, n)),
            dma((ITERS, n)),
            dma((ITERS, n)),
            dma((ITERS, n)),
            dma((1,)),
        ],
        compiler_params=pltpu.CompilerParams(
            collective_id=0, has_side_effects=True, vmem_limit_bytes=48 * 1024 * 1024
        ),
    )(genotype, basis.T)
    return scores.T, block.T


def plain(genotype, basis):
    observed = genotype < 3
    dosage = jnp.where(observed, genotype, 0).astype(jnp.float32)
    allele_sum, called = lax.psum(
        (jnp.sum(dosage, axis=0), jnp.sum(observed.astype(jnp.float32), axis=0)), "samp"
    )
    freq = (allele_sum + 1.0) / (2.0 * called + 2.0)
    scale = 1.0 / jnp.sqrt(2.0 * freq * (1.0 - freq))
    standard = jnp.where(observed, (dosage - 2.0 * freq) * scale, 0.0).astype(jnp.bfloat16)
    total = genotype.shape[0] * lax.axis_size("samp")
    contract = (((0,), (0,)), ((), ()))
    block = basis
    for step in range(ITERS):
        scores = lax.psum(jnp.dot(standard, block, preferred_element_type=jnp.float32), "snp")
        sample_scores = scores.astype(jnp.bfloat16)
        local = lax.dot_general(
            standard, sample_scores, contract, preferred_element_type=jnp.float32
        )
        snp_block = lax.psum(local, "samp") / total
        block = snp_block.astype(jnp.bfloat16)
    return (sample_scores, snp_block)


def solution(mesh):
    n, sides = mesh.shape["samp"], mesh.shape["snp"]

    def per_device(genotype, basis):
        rows, cols = genotype.shape
        fits = (
            sides == 2 and n >= 2 and n & (n - 1) == 0 and cols == n * LANES
            and cols % (8 * LANES) == 0 and rows % LANES == 0 and 2 * rows * n < SHIFT
        )
        return fused(n, genotype, basis) if fits else plain(genotype, basis)

    return jax.shard_map(
        per_device,
        mesh=mesh,
        in_specs=(P("samp", "snp"), P("snp", None)),
        out_specs=(P("samp", None), P("snp", None)),
        check_vma=False,
    )
```

```python
import functools

import jax
import jax.numpy as jnp
from jax import lax
from jax.experimental import pallas as pl
from jax.experimental.pallas import tpu as pltpu
from jax.sharding import PartitionSpec as P

ITERS = 2
LANES = 128
WIDE = 256
SHIFT = 65536
MESH = pl.DeviceIdType.MESH
NT = (((1,), (1,)), ((), ()))


def flipped(me, bits):
    out, step = me, 1
    while step <= bits:
        if bits & step:
            out = out + step * (1 - 2 * lax.rem(me // step, 2))
        step *= 2
    return out


def kernel(
    n, genotype, basis, scores_out, block_out,
    raw, std, hot, stat, table, start, acc, mine, theirs, part, got, full, result,
    load_sem, in_sem, stat_send, stat_recv, score_send, score_recv,
    part_send, part_recv, full_send, full_recv, out_sem,
):
    me = lax.axis_index("samp")
    side = lax.axis_index("snp")
    rows, cols = genotype.shape
    total = rows * n
    blocks = cols // LANES
    groups = blocks // 8
    chunks = cols // WIDE

    barrier = pltpu.get_barrier_semaphore()
    for d in range(1, n):
        pl.semaphore_signal(barrier, inc=1, device_id={"samp": flipped(me, d)}, device_id_type=MESH)
    pl.semaphore_signal(barrier, inc=1, device_id={"snp": 1 - side}, device_id_type=MESH)

    def load(j):
        at = pl.ds(pl.multiple_of(j * LANES, LANES), LANES)
        return pltpu.make_async_copy(genotype.at[:, at], raw.at[j], load_sem.at[j])

    for c in range(blocks):
        load(c).start()
    fetch = pltpu.make_async_copy(basis, start, in_sem)
    fetch.start()

    def count(j, _):
        load(j).wait()
        g = raw[j]
        sums = jnp.sum(jnp.where(g == 3, SHIFT, g), axis=0, keepdims=True)
        std[j] = g.astype(jnp.float32).astype(jnp.bfloat16)
        stat[me, j // 8, pl.ds(lax.rem(j, 8), 1), :] = sums
        return 0

    def stat_copy(h, d):
        peer = flipped(me, d)
        return pltpu.make_async_remote_copy(
            src_ref=stat.at[me, h], dst_ref=stat.at[me, h],
            send_sem=stat_send.at[h, d], recv_sem=stat_recv.at[h, d],
            device_id={"samp": peer}, device_id_type=MESH,
        )

    per_group = blocks // groups
    for h in range(groups):
        lax.fori_loop(h * per_group, (h + 1) * per_group, count, 0)
        if h == 0:
            pl.semaphore_wait(barrier, n)
        for d in reversed(range(1, n)):
            stat_copy(h, d).start()

    def planes(j, _):
        g = std[j]
        one, two, three, none = (jnp.full(g.shape, v, jnp.bfloat16) for v in (1, 2, 3, 0))
        hot[0, j] = jnp.maximum(one - g, none)
        hot[1, j] = jnp.minimum(g, jnp.maximum(two - g, none))
        hot[2, j] = jnp.maximum(jnp.minimum(g - one, three - g), none)
        return 0

    lax.fori_loop(0, blocks, planes, 0)

    for h in range(groups):
        for d in range(1, n):
            stat_copy(h, d).wait_recv()
        packed = stat[0, h]
        for s in range(1, n):
            packed += stat[s, h]
        missing = packed // SHIFT
        allele_sum = (packed - missing * SHIFT).astype(jnp.float32)
        called = (total - missing).astype(jnp.float32)
        freq = (allele_sum + 1.0) / (2.0 * called + 2.0)
        scale = 1.0 / jnp.sqrt(2.0 * freq * (1.0 - freq))
        for k in range(3):
            table[k, h] = (float(k) - 2.0 * freq) * scale

    fetch.wait()

    def standardize(j):
        row = [
            table[k, j // 8, pl.ds(lax.rem(j, 8), 1), :].astype(jnp.bfloat16) for k in range(3)
        ]
        std[j] = hot[0, j] * row[0] + hot[1, j] * row[1] + hot[2, j] * row[2]

    def pair(c):
        return jnp.concatenate([std[2 * c], std[2 * c + 1]], axis=1)

    acc[...] = jnp.zeros_like(acc)

    def first(c, _):
        for half in range(WIDE // LANES):
            standardize(c * (WIDE // LANES) + half)
        at = pl.ds(pl.multiple_of(c * WIDE, WIDE), WIDE)
        acc[...] += lax.dot_general(start[:, at], pair(c), NT, preferred_element_type=jnp.float32)
        return 0

    lax.fori_loop(0, chunks, first, 0)

    sent = []
    for step in range(ITERS):
        last = step == ITERS - 1
        mine[step] = acc[...].astype(jnp.bfloat16)
        swap = pltpu.make_async_remote_copy(
            src_ref=mine.at[step], dst_ref=theirs.at[step],
            send_sem=score_send.at[step], recv_sem=score_recv.at[step],
            device_id={"snp": 1 - side}, device_id_type=MESH,
        )
        swap.start()
        swap.wait_recv()
        scores = (mine[step].astype(jnp.float32) + theirs[step].astype(jnp.float32)).astype(jnp.bfloat16)
        result[...] = scores
        if last:
            score_write = pltpu.make_async_copy(result, scores_out, out_sem.at[0])
            score_write.start()

        def part_copy(owner, step=step):
            return pltpu.make_async_remote_copy(
                src_ref=part.at[step, owner], dst_ref=got.at[step, me],
                send_sem=part_send.at[step, owner], recv_sem=part_recv.at[step, me],
                device_id={"samp": owner}, device_id_type=MESH,
            )

        def part_arrival(sender):
            return pltpu.make_async_remote_copy(
                src_ref=part.at[step, sender], dst_ref=got.at[step, sender],
                send_sem=part_send.at[step, sender], recv_sem=part_recv.at[step, sender],
                device_id={"samp": sender}, device_id_type=MESH,
            )

        per_dot = 4 if n % 4 == 0 else 1
        dots = n // per_dot

        def back(i, _):
            c = lax.rem(me // per_dot + 1 + i, dots)
            wide = jnp.concatenate([std[c * per_dot + r] for r in range(per_dot)], axis=1)
            local = jnp.dot(result[...], wide, preferred_element_type=jnp.float32)
            for r in range(per_dot):
                owner = c * per_dot + r
                part[step, owner] = local[:, r * LANES : (r + 1) * LANES].astype(jnp.bfloat16)

                @pl.when(owner != me)
                def _():
                    part_copy(owner).start()

            return 0

        lax.fori_loop(0, dots, back, 0)

        whole = part[step, me].astype(jnp.float32)
        for d in range(1, n):
            sender = flipped(me, d)
            part_arrival(sender).wait_recv()
            whole += got[step, sender].astype(jnp.float32)
        full[step, me] = (whole / total).astype(jnp.bfloat16)

        def full_copy(peer, slot, step=step):
            return pltpu.make_async_remote_copy(
                src_ref=full.at[step, slot], dst_ref=full.at[step, slot],
                send_sem=full_send.at[step, peer], recv_sem=full_recv.at[step, slot],
                device_id={"samp": peer}, device_id_type=MESH,
            )

        for d in reversed(range(1, n)):
            full_copy(flipped(me, d), me).start()

        if not last:
            acc[...] = jnp.zeros_like(acc)

        def arrive(s):
            @pl.when(s != me)
            def _():
                full_copy(s, s).wait_recv()

        def take(i, _):
            c = lax.rem(me // 2 + i, n // 2)
            for r in range(2):
                arrive(2 * c + r)
            at = pl.ds(pl.multiple_of(c * WIDE, WIDE), WIDE)
            both = jnp.concatenate([full[step, 2 * c], full[step, 2 * c + 1]], axis=1)
            if last:
                block_out[:, at] = both.astype(jnp.float32)
            else:
                acc[...] += lax.dot_general(both, pair(c), NT, preferred_element_type=jnp.float32)
            return 0

        lax.fori_loop(0, n // 2, take, 0)

        sent.append((step, swap))

    for step, swap in sent:
        for d in range(1, n):
            peer = flipped(me, d)
            part_copy(peer, step).wait_send()
            full_copy(peer, me, step).wait_send()
        swap.wait_send()
    for h in range(groups):
        for d in range(1, n):
            stat_copy(h, d).wait_send()
    score_write.wait()


def fused(n, genotype, basis):
    rows, cols = genotype.shape
    width = basis.shape[1]
    blocks = cols // LANES
    dma = pltpu.SemaphoreType.DMA
    scores, block = pl.pallas_call(
        functools.partial(kernel, n),
        out_shape=(
            jax.ShapeDtypeStruct((width, rows), jnp.bfloat16),
            jax.ShapeDtypeStruct((width, cols), jnp.float32),
        ),
        in_specs=[pl.BlockSpec(memory_space=pltpu.HBM)] * 2,
        out_specs=(
            pl.BlockSpec(memory_space=pl.ANY),
            pl.BlockSpec(memory_space=pltpu.VMEM),
        ),
        scratch_shapes=[
            pltpu.VMEM((blocks, rows, LANES), jnp.int32),
            pltpu.VMEM((blocks, rows, LANES), jnp.bfloat16),
            pltpu.VMEM((3, blocks, rows, LANES), jnp.bfloat16),
            pltpu.VMEM((n, blocks // 8, 8, LANES), jnp.int32),
            pltpu.VMEM((3, blocks // 8, 8, LANES), jnp.float32),
            pltpu.VMEM((width, cols), jnp.bfloat16),
            pltpu.VMEM((width, rows), jnp.float32),
            pltpu.VMEM((ITERS, width, rows), jnp.bfloat16),
            pltpu.VMEM((ITERS, width, rows), jnp.bfloat16),
            pltpu.VMEM((ITERS, n, width, LANES), jnp.bfloat16),
            pltpu.VMEM((ITERS, n, width, LANES), jnp.bfloat16),
            pltpu.VMEM((ITERS, n, width, LANES), jnp.bfloat16),
            pltpu.VMEM((width, rows), jnp.bfloat16),
            dma((blocks,)),
            dma,
            dma((blocks // 8, n)),
            dma((blocks // 8, n)),
            dma((ITERS,)),
            dma((ITERS,)),
            dma((ITERS, n)),
            dma((ITERS, n)),
            dma((ITERS, n)),
            dma((ITERS, n)),
            dma((1,)),
        ],
        compiler_params=pltpu.CompilerParams(
            collective_id=0, has_side_effects=True, vmem_limit_bytes=48 * 1024 * 1024
        ),
    )(genotype, basis.T)
    return scores.T, block.T


def plain(genotype, basis):
    observed = genotype < 3
    dosage = jnp.where(observed, genotype, 0).astype(jnp.float32)
    allele_sum, called = lax.psum(
        (jnp.sum(dosage, axis=0), jnp.sum(observed.astype(jnp.float32), axis=0)), "samp"
    )
    freq = (allele_sum + 1.0) / (2.0 * called + 2.0)
    scale = 1.0 / jnp.sqrt(2.0 * freq * (1.0 - freq))
    standard = jnp.where(observed, (dosage - 2.0 * freq) * scale, 0.0).astype(jnp.bfloat16)
    total = genotype.shape[0] * lax.axis_size("samp")
    contract = (((0,), (0,)), ((), ()))
    block = basis
    for step in range(ITERS):
        scores = lax.psum(jnp.dot(standard, block, preferred_element_type=jnp.float32), "snp")
        sample_scores = scores.astype(jnp.bfloat16)
        local = lax.dot_general(
            standard, sample_scores, contract, preferred_element_type=jnp.float32
        )
        snp_block = lax.psum(local, "samp") / total
        block = snp_block.astype(jnp.bfloat16)
    return (sample_scores, snp_block)


def solution(mesh):
    n, sides = mesh.shape["samp"], mesh.shape["snp"]

    def per_device(genotype, basis):
        rows, cols = genotype.shape
        fits = (
            sides == 2 and n >= 2 and n & (n - 1) == 0 and cols == n * LANES
            and cols % (8 * LANES) == 0 and rows % LANES == 0 and 2 * rows * n < SHIFT
        )
        return fused(n, genotype, basis) if fits else plain(genotype, basis)

    return jax.shard_map(
        per_device,
        mesh=mesh,
        in_specs=(P("samp", "snp"), P("snp", None)),
        out_specs=(P("samp", None), P("snp", None)),
        check_vma=False,
    )
```
